16 devices in a mesh: pc: 2 (over z), pr: 8 (over y, x, core).
Axes of the slice: x: 2, y: 2, z: 2, core: 2. Of those that a mesh axis runs over, the one named last changes fastest.
Arguments:
- a_panels: float32 [32768, 2, 64], P('pr', 'pc')
- a_trail: float32 [32768, 3968], P('pr', 'pc')
Outputs:
- output 1: float32 [32768, 2, 64], P('pr', 'pc')
- output 2: float32 [32768, 3968], P('pr', 'pc')
- output 3: float32 [128], replicated
All inputs are finite; a program needn't handle non-finite values.
Results may differ from the reference program's by a relative error of at most 0.001.
Values sent between devices are 32-bit elements.
A program may use at most 1 GiB of HBM per device.

```python
import jax
import jax.numpy as jnp
from jax import lax

TOTAL_ROWS = 32768
TOTAL_COLS = 4096
BLOCK_COLS = 64
NUM_PANELS = 2
PROC_COLS = 2
SHARD_ROWS = 4096

FULL_PRECISION = lax.Precision.HIGHEST
PANEL_WIDTH = NUM_PANELS * BLOCK_COLS
PER_COL = NUM_PANELS // PROC_COLS


def logical_panels(panels_in):
    n_rows = panels_in.shape[0]
    block_grid = panels_in.reshape(n_rows, PROC_COLS, PER_COL, BLOCK_COLS)
    return block_grid.transpose(0, 2, 1, 3).reshape(n_rows, PANEL_WIDTH)


def stored_panels(flat_cols):
    n_rows = flat_cols.shape[0]
    block_grid = flat_cols.reshape(n_rows, PER_COL, PROC_COLS, BLOCK_COLS)
    return block_grid.transpose(0, 2, 1, 3).reshape(n_rows, NUM_PANELS, BLOCK_COLS)


def setup_inputs(seed: int = 0) -> dict:
    key_base, key_rows, key_cols, key_sign = jax.random.split(jax.random.key(seed), 4)
    n_shards = TOTAL_ROWS // SHARD_ROWS
    n_blocks = TOTAL_COLS // BLOCK_COLS
    base_vals = jax.random.normal(key_base, (TOTAL_ROWS, TOTAL_COLS), jnp.float32)
    shard_scale = jnp.exp2(jax.random.uniform(key_rows, (n_shards,), jnp.float32, -2.0, 2.0))
    block_scale = jnp.exp2(jax.random.uniform(key_cols, (n_blocks,), jnp.float32, -1.0, 1.0))
    row_scale = jnp.repeat(shard_scale, SHARD_ROWS, total_repeat_length=TOTAL_ROWS)
    col_scale = jnp.repeat(block_scale, BLOCK_COLS, total_repeat_length=TOTAL_COLS)
    full_mat = base_vals * row_scale[:, None] * col_scale[None, :]
    diag_ids = jnp.arange(PANEL_WIDTH)
    diag_signs = jnp.where(jax.random.bernoulli(key_sign, 0.5, (PANEL_WIDTH,)), 1.0, -1.0)
    diag_boost = 8.0 * diag_signs * row_scale[:PANEL_WIDTH] * col_scale[:PANEL_WIDTH]
    full_mat = full_mat.at[diag_ids, diag_ids].add(diag_boost) * (TOTAL_ROWS ** -0.25)
    return {'a_panels': stored_panels(full_mat[:, :PANEL_WIDTH]), 'a_trail': full_mat[:, PANEL_WIDTH:]}


def factor_panel(panel_blk):
    n_rows, blk_width = panel_blk.shape
    row_ids = jnp.arange(n_rows)
    col_ids = jnp.arange(blk_width)

    def column_step(j, carry):
        fac_panel, tau_vec = carry
        column = lax.dynamic_slice_in_dim(fac_panel, j, 1, axis=1)[:, 0]
        below_diag = row_ids > j
        at_diag = row_ids == j
        sum_sq = jnp.sum(jnp.where(row_ids >= j, column * column, 0.0))
        diag_val = jnp.sum(jnp.where(at_diag, column, 0.0))
        col_norm = jnp.sqrt(sum_sq)
        beta_val = jnp.where(diag_val >= 0.0, -col_norm, col_norm)
        tau_j = (beta_val - diag_val) / beta_val
        house_vec = jnp.where(below_diag, column / (diag_val - beta_val), jnp.where(at_diag, 1.0, 0.0))
        proj_row = jnp.dot(house_vec, fac_panel, precision=FULL_PRECISION, preferred_element_type=jnp.float32)
        proj_row = jnp.where(col_ids > j, tau_j * proj_row, 0.0)
        fac_panel = fac_panel - house_vec[:, None] * proj_row[None, :]
        new_col = jnp.where(below_diag, house_vec, jnp.where(at_diag, beta_val, column))
        fac_panel = jnp.where(col_ids[None, :] == j, new_col[:, None], fac_panel)
        tau_vec = jnp.where(col_ids == j, tau_j, tau_vec)
        return fac_panel, tau_vec

    return lax.fori_loop(0, blk_width, column_step, (panel_blk, jnp.zeros((blk_width,), panel_blk.dtype)))


def unit_lower(fac_panel):
    row_ids = jnp.arange(fac_panel.shape[0])
    col_ids = jnp.arange(fac_panel.shape[1])
    return jnp.where(row_ids[:, None] > col_ids[None, :], fac_panel, jnp.where(row_ids[:, None] == col_ids[None, :], 1.0, 0.0))


def build_t(gram_mat, tau_vec):
    blk_width = tau_vec.shape[0]
    col_ids = jnp.arange(blk_width)

    def t_step(j, t_mat):
        g_col = jnp.where(col_ids < j, lax.dynamic_slice_in_dim(gram_mat, j, 1, axis=1)[:, 0], 0.0)
        tau_j = jnp.sum(jnp.where(col_ids == j, tau_vec, 0.0))
        new_col = -tau_j * jnp.dot(t_mat, g_col, precision=FULL_PRECISION, preferred_element_type=jnp.float32)
        new_col = jnp.where(col_ids == j, tau_j, new_col)
        return jnp.where(col_ids[None, :] == j, new_col[:, None], t_mat)

    return lax.fori_loop(0, blk_width, t_step, jnp.zeros((blk_width, blk_width), gram_mat.dtype))


def reference(a_panels, a_trail):
    work_mat = jnp.concatenate([logical_panels(a_panels), a_trail], axis=1)
    tau_parts = []
    for k in range(NUM_PANELS):
        first_col = k * BLOCK_COLS
        end_col = first_col + BLOCK_COLS
        fac_panel, tau_vec = factor_panel(work_mat[first_col:, first_col:end_col])
        v_mat = unit_lower(fac_panel)
        gram_mat = jnp.dot(v_mat.T, v_mat, precision=FULL_PRECISION, preferred_element_type=jnp.float32)
        t_mat = build_t(gram_mat, tau_vec)
        trail_cols = work_mat[first_col:, end_col:]
        inner_prod = jnp.dot(v_mat.T, trail_cols, precision=FULL_PRECISION, preferred_element_type=jnp.float32)
        inner_prod = jnp.dot(t_mat.T, inner_prod, precision=FULL_PRECISION, preferred_element_type=jnp.float32)
        trail_cols = trail_cols - jnp.dot(v_mat, inner_prod, precision=FULL_PRECISION, preferred_element_type=jnp.float32)
        work_mat = work_mat.at[first_col:, first_col:end_col].set(fac_panel)
        work_mat = work_mat.at[first_col:, end_col:].set(trail_cols)
        tau_parts.append(tau_vec)
    return stored_panels(work_mat[:, :PANEL_WIDTH]), work_mat[:, PANEL_WIDTH:], jnp.concatenate(tau_parts)
```

```python
import jax
import jax.numpy as jnp
from jax import lax
from jax.experimental import pallas as pl
from jax.experimental.pallas import tpu as pltpu
from jax.sharding import PartitionSpec as P

FULL_PRECISION = lax.Precision.HIGHEST
MESH = pl.DeviceIdType.MESH
ROWS, NB, NP, TRAIL = 4096, 64, 128, 1984
NPR = 8
LANES = 1024
NCH = ROWS // LANES
OWN = TRAIL // NPR
MROWS = 496
MSG = NP + 8


def mat_prod(form, left, right):
    return jnp.einsum(form, left, right, precision=FULL_PRECISION, preferred_element_type=jnp.float32)


def fdot(a, b):
    return jnp.dot(a, b, precision=FULL_PRECISION, preferred_element_type=jnp.float32)


def bdot(a, b):
    return jnp.dot(a, b, preferred_element_type=jnp.float32)


def split3(x):
    hi = x.astype(jnp.bfloat16)
    rest = x - hi.astype(jnp.float32)
    mid = rest.astype(jnp.bfloat16)
    low = (rest - mid.astype(jnp.float32)).astype(jnp.bfloat16)
    return hi, mid, low


def dot_parts(x, pieces):
    hi, mid, low = split3(x)
    d1 = bdot(hi, pieces)
    d2 = bdot(mid, pieces[:, :2 * NP])
    d3 = bdot(low, pieces[:, :NP])
    return d1[:, :NP] + ((d1[:, NP:2 * NP] + d2[:, :NP]) + ((d1[:, 2 * NP:] + d3) + d2[:, NP:]))


def unit_tri_inv(strict, eye):
    inv = eye + strict
    power = strict
    for _ in range(6):
        power = fdot(power, power)
        inv = inv + fdot(inv, power)
    return inv


def eye_of(n):
    return lax.broadcasted_iota(jnp.int32, (n, n), 0) == lax.broadcasted_iota(jnp.int32, (n, n), 1)


def factor_steps(h_s, b_s, r_s, u_s, row0, start, stop):
    n_rows = NP - row0
    lane1 = lax.broadcasted_iota(jnp.int32, (1, NP), 1)
    lane = lax.broadcasted_iota(jnp.int32, (n_rows, NP), 1)

    def step(j, carry):
        idx = jnp.full((n_rows, NP), j, jnp.int32)
        idx8 = jnp.full((8, NP), j, jnp.int32)
        hrow = h_s[pl.ds(j, 1), :]
        brow = b_s[pl.ds(j, 1), :]
        hjj = jnp.take_along_axis(jnp.broadcast_to(hrow, (8, NP)), idx8, axis=1)[:1]
        alpha = jnp.take_along_axis(jnp.broadcast_to(brow, (8, NP)), idx8, axis=1)[:1]
        hcol = jnp.take_along_axis(h_s[row0:, :], idx, axis=1)
        bcol = jnp.take_along_axis(b_s[row0:, :], idx, axis=1)
        root = lax.rsqrt(hjj)
        root = root * (1.5 - 0.5 * hjj * root * root)
        beta = jnp.where(alpha >= 0.0, -hjj * root, hjj * root)
        invb = jnp.where(alpha >= 0.0, -root, root)
        invd = 1.0 / (alpha - beta)
        keep = lane1 >= j
        rrow = jnp.where(keep, hrow * invb, 0.0)
        urow = jnp.where(keep, brow - rrow, 0.0)
        r_s[pl.ds(j, 1), :] = rrow
        u_s[pl.ds(j, 1), :] = urow
        h_s[row0:, :] = h_s[row0:, :] - hcol * (rrow * invb)
        vcol = bcol * invd
        b_s[row0:, :] = jnp.where(lane == j, vcol, b_s[row0:, :] - vcol * urow)
        return carry

    lax.fori_loop(start, stop, step, 0)


def reduce_kernel(panel_hbm, trail_hbm, pt_out, wt_out, zt_out, tops_out, tau_out, bad_out,
                  cbuf, pt, pp, gown, gin, gsum, ptop, ct, part, rin, part2, rsum, st, h_s, b_s, r_s, u_s, cmx,
                  csem, psem, zsend, zrecv, osem, gsend, grecv, tsend, trecv, csend, crecv, r1sem, r2send, r2recv,
                  casend, carecv, sasend, sarecv, msem):
    me = lax.axis_index('pr')
    q = lax.axis_index('pc')
    core = lax.rem(me, 2)
    chip = (me - core) // 2
    twin = me + 1 - 2 * core
    partner = {'pc': 1 - q}
    mine = pl.ds(pl.multiple_of(q * NB, NB), NB)
    theirs = pl.ds(pl.multiple_of((1 - q) * NB, NB), NB)

    def remote(src, dst, s_sem, r_sem, dev):
        return pltpu.make_async_remote_copy(src_ref=src, dst_ref=dst, send_sem=s_sem, recv_sem=r_sem, device_id=dev, device_id_type=MESH)

    def lanes(c):
        return pl.ds(c * LANES, LANES)

    def load_trail(c):
        return pltpu.make_async_copy(trail_hbm.at[:, lanes(c)], cbuf.at[:, lanes(c)], csem.at[c])

    def load_panel(c):
        return pltpu.make_async_copy(panel_hbm.at[:, lanes(c)], pt.at[mine, lanes(c)], psem.at[c])

    def send_panel(c):
        return remote(pt.at[mine, lanes(c)], pt.at[mine, lanes(c)], zsend.at[c], zrecv.at[c], partner)

    def recv_panel(c):
        return remote(pt.at[theirs, lanes(c)], pt.at[theirs, lanes(c)], zsend.at[c], zrecv.at[c], partner)

    for c in range(NCH):
        load_panel(c).start()
    for c in range(NCH):
        load_trail(c).start()

    barrier = pltpu.get_barrier_semaphore()
    pl.semaphore_signal(barrier, inc=1, device_id=partner, device_id_type=MESH)
    for d in range(1, NPR):
        pl.semaphore_signal(barrier, inc=1, device_id={'pr': lax.rem(me + d, NPR)}, device_id_type=MESH)
    pl.semaphore_wait(barrier, NPR)
    for c in range(NCH):
        load_panel(c).wait()
        send_panel(c).start()

    def gather_start(buf, ssem, rsem):
        for d in range(4):
            dev = twin if d == 0 else lax.rem(me + 2 * d, NPR)
            remote(buf.at[me], buf.at[me], ssem.at[d], rsem.at[me], {'pr': dev}).start()

    def gather_forward(buf, ssem, rsem):
        for d in range(1, 4):
            src = lax.rem(me + NPR - 2 * d, NPR)
            remote(buf.at[src], buf.at[src], ssem.at[3 + d], rsem.at[src], {'pr': twin}).wait_recv()
            remote(buf.at[src], buf.at[src], ssem.at[3 + d], rsem.at[src], {'pr': twin}).start()

    def gather_wait(buf, ssem, rsem):
        for d in range(4):
            src = lax.rem(twin + NPR - 2 * d, NPR)
            remote(buf.at[src], buf.at[src], ssem.at[d], rsem.at[src], {'pr': twin}).wait_recv()

    def gather_end(buf, ssem, rsem):
        for d in range(7):
            remote(buf.at[me], buf.at[me], ssem.at[d], rsem.at[me], {'pr': twin}).wait_send()

    def share_top(i):
        return remote(pt.at[:, pl.ds(0, NP)], ptop, tsend.at[i], trecv, {'pr': i})

    def scatter_top(i):
        return remote(cbuf.at[pl.ds(i * OWN, OWN), pl.ds(0, NP)], ct.at[i], csend.at[i], crecv, {'pr': i})

    part[...] = jnp.zeros_like(part)
    gown[...] = jnp.zeros_like(gown)

    def make_pieces(c):
        hi, mid, low = split3(pt[:, lanes(c)].T)
        pp[:, :NP] = hi
        pp[:, NP:2 * NP] = mid
        pp[:, 2 * NP:] = low
        gown[:NP, :] += dot_parts(pt[:, lanes(c)], pp[...])

    def product(c, first, last):
        def rows_step(m, carry):
            rows = pl.ds(pl.multiple_of(m * MROWS, MROWS), MROWS)
            got = dot_parts(cbuf[rows, lanes(c)], pp[...])
            part[m] += got.reshape(2, OWN, NP)
            return carry

        lax.fori_loop(first, last, rows_step, 0)

    cmax = jnp.zeros((8, LANES), jnp.float32)
    for c in range(NCH):
        load_trail(c).wait()
        if c == 0:
            @pl.when(me == 0)
            def _():
                ct[0] = cbuf[:OWN, :NP]
                for i in range(1, NPR):
                    scatter_top(i).start()

        def largest(m, acc):
            x = cbuf[pl.ds(pl.multiple_of(m * OWN, OWN), OWN), lanes(c)]
            return jnp.maximum(acc, jnp.max(jnp.abs(x).reshape(OWN // 8, 8, LANES), axis=0))

        cmax = lax.fori_loop(0, NPR, largest, cmax)
        if c == 1:
            @pl.when(me != 0)
            def _():
                remote(ct.at[me], ct.at[me], csend.at[0], crecv, {'pr': 0}).wait_recv()

            gather_start(ct, casend, carecv)
        if c == 3:
            gather_forward(ct, casend, carecv)
        recv_panel(c).wait_recv()
        if c == 0:
            @pl.when(me == 0)
            def _():
                ptop[...] = pt[:, :NP]
                for i in range(1, NPR):
                    share_top(i).start()
        make_pieces(c)
        if c < NCH - 1:
            product(c, 0, 4)

    big = jnp.max(jnp.max(cmax, axis=1, keepdims=True), axis=0, keepdims=True)
    gown[NP:, :] = jnp.broadcast_to(big, (8, NP))

    gcopy = remote(gown, gin, gsend.at[0], grecv.at[4], {'pr': twin})
    gcopy.start()
    pt_copy = pltpu.make_async_copy(pt, pt_out, osem)
    pt_copy.start()
    product(NCH - 1, 0, 2)
    gcopy.wait()
    gsum[chip, :NP, :] = gown[:NP, :] + gin[:NP, :]
    gsum[chip, NP:, :] = jnp.maximum(gown[NP:, :], gin[NP:, :])

    def send_gram(d):
        return remote(gsum.at[chip], gsum.at[chip], gsend.at[d], grecv.at[chip], {'pr': lax.rem(me + 2 * d, NPR)})

    for d in range(1, 4):
        send_gram(d).start()
    product(NCH - 1, 2, 4)

    scopy = remote(part.at[:, 1 - core], rin, r1sem.at[0], r1sem.at[1], {'pr': twin})
    scopy.start()

    @pl.when(me != 0)
    def _():
        remote(ptop, ptop, tsend.at[0], trecv, {'pr': 0}).wait_recv()

    for d in range(1, 4):
        src = lax.rem(chip + 4 - d, 4)
        remote(gsum.at[src], gsum.at[src], gsend.at[d], grecv.at[src], {'pr': twin}).wait_recv()
    gram = ((gsum[0, :NP, :] + gsum[1, :NP, :]) + gsum[2, :NP, :]) + gsum[3, :NP, :]
    cmx[0] = jnp.maximum(jnp.maximum(gsum[0, NP:, :], gsum[1, NP:, :]), jnp.maximum(gsum[2, NP:, :], gsum[3, NP:, :]))
    mcopy = remote(cmx.at[0], cmx.at[1], msem.at[0], msem.at[1], partner)
    mcopy.start()

    eyeb = eye_of(NP)
    eye = jnp.where(eyeb, 1.0, 0.0)
    row_id = lax.broadcasted_iota(jnp.int32, (NP, NP), 0)
    col_id = lax.broadcasted_iota(jnp.int32, (NP, NP), 1)

    def newton_rsqrt(x):
        y = lax.rsqrt(x)
        return y * (1.5 - 0.5 * x * y * y)

    gdiag = jnp.where(eyeb, gram, 0.0)
    g_row = jnp.sum(gdiag, axis=0, keepdims=True)
    g_col = jnp.sum(gdiag, axis=1, keepdims=True)
    n_row, n_col = newton_rsqrt(g_row), newton_rsqrt(g_col)
    h_s[...] = (gram * n_row) * n_col
    b_s[...] = ptop[...].T * n_row
    factor_steps(h_s, b_s, r_s, u_s, 0, 0, 16)

    scopy.wait()
    for s in range(4):
        part2[s] = part[s, core] + rin[s]

    def scatter_part(d):
        to = lax.rem(chip + d, 4)
        return remote(part2.at[to], rsum.at[chip], r2send.at[d], r2recv.at[chip], {'pr': 2 * to + core})

    for d in range(1, 4):
        scatter_part(d).start()
    factor_steps(h_s, b_s, r_s, u_s, 0, 16, 64)
    rsum[chip] = part2[chip]
    for d in range(1, 4):
        src = lax.rem(chip + 4 - d, 4)
        remote(part2.at[src], rsum.at[src], r2send.at[d], r2recv.at[src], {'pr': twin}).wait_recv()
    st[me] = ((rsum[0] + rsum[1]) + rsum[2]) + rsum[3]
    gather_start(st, sasend, sarecv)
    factor_steps(h_s, b_s, r_s, u_s, NB, 64, 120)
    gather_forward(st, sasend, sarecv)
    gather_wait(ct, casend, carecv)
    factor_steps(h_s, b_s, r_s, u_s, NB, 120, 128)

    rmat, umat = r_s[...], u_s[...]
    lstrict = jnp.where(row_id > col_id, b_s[...], 0.0)
    lmat = eye + lstrict

    def upper_inv(mat):
        diag = jnp.where(eyeb, mat, 0.0)
        d_row = 1.0 / jnp.sum(diag, axis=0, keepdims=True)
        d_col = 1.0 / jnp.sum(diag, axis=1, keepdims=True)
        return unit_tri_inv(jnp.where(col_id > row_id, -(mat * d_col), 0.0), eye) * d_row

    rinv = upper_inv(rmat)
    uinv = upper_inv(umat)
    linv = unit_tri_inv(-lstrict, eye)
    wt_out[...] = (uinv * n_col).T
    linv_t = linv.T
    m2_t = (fdot(linv, rinv.T) * n_row).T
    tau_out[...] = jnp.sum(jnp.where(eyeb, -umat / rmat, 0.0), axis=0, keepdims=True)
    tops_out[:NP, :] = lmat.T
    tops_out[NP:, :] = jnp.where(row_id > col_id, lmat, rmat * (g_row * n_row)).T

    mcopy.wait()
    c_top = jnp.max(jnp.maximum(cmx[0], cmx[1]), axis=1, keepdims=True)[:1]
    g_max = jnp.max(g_row, axis=1, keepdims=True)
    g_min = jnp.min(g_row, axis=1, keepdims=True)

    def total_of(x):
        return jnp.sum(jnp.sum(x, axis=1, keepdims=True), axis=0, keepdims=True)

    resid = total_of(jnp.abs(fdot(rinv, rmat) - eye) + jnp.abs(fdot(uinv, umat) - eye) + jnp.abs(fdot(linv, lmat) - eye))
    cond = total_of(rinv * rinv + uinv * uinv + linv * linv)
    good = (g_max < 1e12) & (g_min > 1e-12) & (resid < 1e-3) & (cond < 2048.0)
    good = good & (c_top < 1e26) & ((c_top > 1e-20) | (c_top == 0.0))
    bad_out[...] = jnp.broadcast_to(jnp.where(good, 0.0, 1.0), (8, NP))

    gather_wait(st, sasend, sarecv)

    def make_z(i, carry):
        zt_out[pl.ds(pl.multiple_of(i * OWN, OWN), OWN), :] = fdot(ct[i], linv_t) - fdot(st[i], m2_t)
        return carry

    lax.fori_loop(0, NPR, make_z, 0)

    pt_copy.wait()
    for c in range(NCH):
        send_panel(c).wait_send()
    gather_end(ct, casend, carecv)
    gather_end(st, sasend, sarecv)
    for d in range(1, 4):
        send_gram(d).wait_send()
        scatter_part(d).wait_send()

    @pl.when(me == 0)
    def _():
        for i in range(1, NPR):
            share_top(i).wait_send()
            scatter_top(i).wait_send()


def reduce_call(panel_t, trail_t):
    f32 = jnp.float32
    dma = pltpu.SemaphoreType.DMA
    vmem = pl.BlockSpec(memory_space=pltpu.VMEM)
    hbm = pl.BlockSpec(memory_space=pl.ANY)
    return pl.pallas_call(
        reduce_kernel,
        out_shape=(
            jax.ShapeDtypeStruct((NP, ROWS), f32), jax.ShapeDtypeStruct((NP, NP), f32), jax.ShapeDtypeStruct((TRAIL, NP), f32),
            jax.ShapeDtypeStruct((2 * NP, NP), f32), jax.ShapeDtypeStruct((1, NP), f32), jax.ShapeDtypeStruct((8, NP), f32)),
        in_specs=[hbm, hbm],
        out_specs=(hbm, vmem, vmem, vmem, vmem, vmem),
        scratch_shapes=[
            pltpu.VMEM((TRAIL, ROWS), f32), pltpu.VMEM((NP, ROWS), f32), pltpu.VMEM((LANES, 3 * NP), jnp.bfloat16),
            pltpu.VMEM((MSG, NP), f32), pltpu.VMEM((MSG, NP), f32), pltpu.VMEM((4, MSG, NP), f32), pltpu.VMEM((NP, NP), f32),
            pltpu.VMEM((NPR, OWN, NP), f32), pltpu.VMEM((4, 2, OWN, NP), f32), pltpu.VMEM((4, OWN, NP), f32), pltpu.VMEM((4, OWN, NP), f32),
            pltpu.VMEM((4, OWN, NP), f32), pltpu.VMEM((NPR, OWN, NP), f32),
            pltpu.VMEM((NP, NP), f32), pltpu.VMEM((NP, NP), f32), pltpu.VMEM((NP, NP), f32), pltpu.VMEM((NP, NP), f32), pltpu.VMEM((2, 8, NP), f32),
            dma((NCH,)), dma((NCH,)), dma((NCH,)), dma((NCH,)), dma(()), dma((4,)), dma((5,)), dma((NPR,)), dma(()), dma((NPR,)), dma(()),
            dma((2,)), dma((4,)), dma((4,)), dma((7,)), dma((NPR,)), dma((7,)), dma((NPR,)), dma((2,))],
        compiler_params=pltpu.CompilerParams(collective_id=0, has_side_effects=True, vmem_limit_bytes=67043328),
        name='reduce',
    )(panel_t, trail_t)


UL = 512


def update_kernel(pt_ref, wt_ref, zt_ref, tops_ref, c_ref, o_ref, pan_ref, zcat, vcat):
    first = pl.program_id(0) == 0
    q = lax.axis_index('pc')

    @pl.when(first)
    def _():
        zh, zm, zl = split3(zt_ref[...])
        for n, piece in enumerate((zh, zh, zm, zm, zl, zh)):
            zcat[:, n * NP:(n + 1) * NP] = piece

    v = fdot(wt_ref[...], pt_ref[...])
    at_top = first & (lax.axis_index('pr') == 0)
    lane = lax.broadcasted_iota(jnp.int32, (NP, UL), 1)
    inside = (lane < NP) & at_top
    pad = jnp.zeros((NP, UL - NP), jnp.float32)
    stored = jnp.where(inside, jnp.concatenate([tops_ref[NP:, :], pad], axis=1), v)
    v = jnp.where(inside, jnp.concatenate([tops_ref[:NP, :], pad], axis=1), v)
    pan_ref[...] = jnp.where(q == 0, stored[:NB], stored[NB:])
    vh, vm, vl = split3(v)
    for n, piece in enumerate((vh, vm, vh, vm, vh, vl)):
        vcat[n * NP:(n + 1) * NP, :] = piece

    def rows_step(m, carry):
        rows = pl.ds(pl.multiple_of(m * MROWS, MROWS), MROWS)
        o_ref[rows, :] = c_ref[rows, :] - bdot(zcat[rows, :], vcat[...])
        return carry

    lax.fori_loop(0, TRAIL // MROWS, rows_step, 0)


def update_call(pt, wt, zt, tops, trail_t):
    f32 = jnp.float32
    return pl.pallas_call(
        update_kernel,
        out_shape=(jax.ShapeDtypeStruct((TRAIL, ROWS), f32), jax.ShapeDtypeStruct((NB, ROWS), f32)),
        grid=(ROWS // UL,),
        in_specs=[pl.BlockSpec((NP, UL), lambda i: (0, i)), pl.BlockSpec((NP, NP), lambda i: (0, 0)), pl.BlockSpec((TRAIL, NP), lambda i: (0, 0)),
                  pl.BlockSpec((2 * NP, NP), lambda i: (0, 0)), pl.BlockSpec((TRAIL, UL), lambda i: (0, i))],
        out_specs=(pl.BlockSpec((TRAIL, UL), lambda i: (0, i)), pl.BlockSpec((NB, UL), lambda i: (0, i))),
        scratch_shapes=[pltpu.VMEM((TRAIL, 6 * NP), jnp.bfloat16), pltpu.VMEM((6 * NP, UL), jnp.bfloat16)],
        compiler_params=pltpu.CompilerParams(dimension_semantics=('arbitrary',), vmem_limit_bytes=40 << 20),
        name='update',
    )(pt, wt, zt, tops, trail_t)


def sum_rows(x):
    for bit in (1, 2, 4):
        x = x + lax.ppermute(x, 'pr', [(i, i ^ bit) for i in range(NPR)])
    return x


def from_owner(x, owner):
    x = jnp.where(lax.axis_index('pc') == owner, x, 0.0)
    return x + lax.ppermute(x, 'pc', [(0, 1), (1, 0)])


def factor_panel(panel_blk, row_ids, first_row):
    col_ids = jnp.arange(NB)

    def column_step(j, carry):
        fac_panel, tau_vec = carry
        diag_row = first_row + j
        column = lax.dynamic_slice_in_dim(fac_panel, j, 1, axis=1)[:, 0]
        below_diag = row_ids > diag_row
        at_diag = row_ids == diag_row
        stats = sum_rows(jnp.stack([jnp.sum(jnp.where(row_ids >= diag_row, column * column, 0.0)), jnp.sum(jnp.where(at_diag, column, 0.0))]))
        diag_val = stats[1]
        col_norm = jnp.sqrt(stats[0])
        beta_val = jnp.where(diag_val >= 0.0, -col_norm, col_norm)
        tau_j = (beta_val - diag_val) / beta_val
        house_vec = jnp.where(below_diag, column / (diag_val - beta_val), jnp.where(at_diag, 1.0, 0.0))
        proj_row = sum_rows(jnp.sum(house_vec[:, None] * fac_panel, axis=0))
        proj_row = jnp.where(col_ids > j, tau_j * proj_row, 0.0)
        fac_panel = fac_panel - house_vec[:, None] * proj_row[None, :]
        new_col = jnp.where(below_diag, house_vec, jnp.where(at_diag, beta_val, column))
        fac_panel = jnp.where(col_ids[None, :] == j, new_col[:, None], fac_panel)
        return fac_panel, jnp.where(col_ids == j, tau_j, tau_vec)

    return lax.fori_loop(0, NB, column_step, (panel_blk, jnp.zeros((NB,), jnp.float32)))


def build_t(gram_mat, tau_vec):
    col_ids = jnp.arange(NB)

    def t_step(j, t_mat):
        g_col = jnp.where(col_ids < j, lax.dynamic_slice_in_dim(gram_mat, j, 1, axis=1)[:, 0], 0.0)
        tau_j = jnp.sum(jnp.where(col_ids == j, tau_vec, 0.0))
        new_col = jnp.where(col_ids == j, tau_j, -tau_j * jnp.sum(t_mat * g_col[None, :], axis=1))
        return jnp.where(col_ids[None, :] == j, new_col[:, None], t_mat)

    return lax.fori_loop(0, NB, t_step, jnp.zeros((NB, NB), jnp.float32))


def by_columns(panel, trail):
    col_idx = lax.axis_index('pc')
    row_ids = lax.axis_index('pr') * ROWS + jnp.arange(ROWS)
    v_parts, z_parts, taus = [], [], []
    for k in range(2):
        fac_panel, tau_vec = factor_panel(panel, row_ids, k * NB)
        diag = k * NB + jnp.arange(NB)
        v_mat = jnp.where(row_ids[:, None] > diag[None, :], fac_panel, jnp.where(row_ids[:, None] == diag[None, :], 1.0, 0.0))
        v_mat = from_owner(v_mat, k)
        tau_vec = from_owner(tau_vec, k)
        t_mat = build_t(sum_rows(mat_prod('rb,rc->bc', v_mat, v_mat)), tau_vec)
        inner = mat_prod('bd,bc->dc', t_mat, sum_rows(mat_prod('rb,rc->bc', v_mat, trail)))
        if k == 0:
            trail = trail - mat_prod('rd,dc->rc', v_mat, inner)
            near = mat_prod('bd,bc->dc', t_mat, sum_rows(mat_prod('rb,rc->bc', v_mat, panel)))
            later = panel - mat_prod('rd,dc->rc', v_mat, near)
            panel = jnp.where(col_idx == 0, fac_panel, later)
        else:
            panel = jnp.where(col_idx == 1, fac_panel, panel)
        v_parts.append(v_mat)
        z_parts.append(inner)
        taus.append(tau_vec)
    v_t = jnp.concatenate(v_parts, axis=1).T
    top = panel[:NP].T
    tops = jnp.concatenate([v_t[:, :NP], top, top], axis=0)
    return v_t, jnp.eye(NP, dtype=jnp.float32), jnp.concatenate(z_parts, axis=0).T, tops, jnp.concatenate(taus)[None, :]


def solution(mesh):
    def local_run(panels_loc, trail_loc):
        panel_t = panels_loc.reshape(ROWS, NB).T
        trail_t = trail_loc.T
        pt, wt, zt, tops, tau, bad = reduce_call(panel_t, trail_t)

        def direct(pt, wt, zt, tops, tau, trail_t, panel_t):
            return update_call(pt, wt, zt, tops, trail_t) + (tau,)

        def again(pt, wt, zt, tops, tau, trail_t, panel_t):
            pt, wt, zt, tops, tau = by_columns(panel_t.T, trail_t.T)
            return update_call(pt, wt, zt, tops, trail_t) + (tau,)

        trail_new, pan, tau = lax.cond(bad[0, 0] > 0.0, again, direct, pt, wt, zt, tops, tau, trail_t, panel_t)
        return pan.T.reshape(ROWS, 1, NB), trail_new.T, tau.reshape(NP)

    return jax.shard_map(local_run, mesh=mesh, in_specs=(P('pr', 'pc', None), P('pr', 'pc')), out_specs=(P('pr', 'pc', None), P('pr', 'pc'), P()), check_vma=False)
```

```python
import jax
import jax.numpy as jnp
from jax import lax
from jax.experimental import pallas as pl
from jax.experimental.pallas import tpu as pltpu
from jax.sharding import PartitionSpec as P

FULL_PRECISION = lax.Precision.HIGHEST
MESH = pl.DeviceIdType.MESH
ROWS, NB, NP, TRAIL = 4096, 64, 128, 1984
NPR = 8
LANES = 1024
NCH = ROWS // LANES
AUX0, ALL = TRAIL, TRAIL + NP
WT0, TOP0, TOP1, TAU0, BAD0 = (16 * NP, 17 * NP, 18 * NP, 19 * NP, 20 * NP)
OWN = TRAIL // NPR
MROWS = 496
MSG = NP + 8


def mat_prod(form, left, right):
    return jnp.einsum(form, left, right, precision=FULL_PRECISION, preferred_element_type=jnp.float32)


def fdot(a, b):
    return jnp.dot(a, b, precision=FULL_PRECISION, preferred_element_type=jnp.float32)


def bdot(a, b):
    return jnp.dot(a, b, preferred_element_type=jnp.float32)


def split3(x):
    hi = x.astype(jnp.bfloat16)
    rest = x - hi.astype(jnp.float32)
    mid = rest.astype(jnp.bfloat16)
    low = (rest - mid.astype(jnp.float32)).astype(jnp.bfloat16)
    return hi, mid, low


def dot_parts(x, pieces):
    hi, mid, low = split3(x)
    d1 = bdot(hi, pieces)
    d2 = bdot(mid, pieces[:, :2 * NP])
    d3 = bdot(low, pieces[:, :NP])
    return d1[:, :NP] + ((d1[:, NP:2 * NP] + d2[:, :NP]) + ((d1[:, 2 * NP:] + d3) + d2[:, NP:]))


def unit_tri_inv(strict, eye):
    inv = eye + strict
    power = strict
    for _ in range(6):
        power = fdot(power, power)
        inv = inv + fdot(inv, power)
    return inv


def eye_of(n):
    return lax.broadcasted_iota(jnp.int32, (n, n), 0) == lax.broadcasted_iota(jnp.int32, (n, n), 1)


def factor_steps(h_s, b_s, r_s, u_s, row0, start, stop):
    n_rows = NP - row0
    lane1 = lax.broadcasted_iota(jnp.int32, (1, NP), 1)
    lane = lax.broadcasted_iota(jnp.int32, (n_rows, NP), 1)

    def step(j, carry):
        idx = jnp.full((n_rows, NP), j, jnp.int32)
        idx8 = jnp.full((8, NP), j, jnp.int32)
        hrow = h_s[pl.ds(j, 1), :]
        brow = b_s[pl.ds(j, 1), :]
        hjj = jnp.take_along_axis(jnp.broadcast_to(hrow, (8, NP)), idx8, axis=1)[:1]
        alpha = jnp.take_along_axis(jnp.broadcast_to(brow, (8, NP)), idx8, axis=1)[:1]
        hcol = jnp.take_along_axis(h_s[row0:, :], idx, axis=1)
        bcol = jnp.take_along_axis(b_s[row0:, :], idx, axis=1)
        root = lax.rsqrt(hjj)
        root = root * (1.5 - 0.5 * hjj * root * root)
        beta = jnp.where(alpha >= 0.0, -hjj * root, hjj * root)
        invb = jnp.where(alpha >= 0.0, -root, root)
        invd = 1.0 / (alpha - beta)
        keep = lane1 >= j
        rrow = jnp.where(keep, hrow * invb, 0.0)
        urow = jnp.where(keep, brow - rrow, 0.0)
        r_s[pl.ds(j, 1), :] = rrow
        u_s[pl.ds(j, 1), :] = urow
        h_s[row0:, :] = h_s[row0:, :] - hcol * (rrow * invb)
        vcol = bcol * invd
        b_s[row0:, :] = jnp.where(lane == j, vcol, b_s[row0:, :] - vcol * urow)
        return carry

    lax.fori_loop(start, stop, step, 0)


def reduce_kernel(panel_hbm, trail_hbm, out, pt_out,
                  pt, pp, gown, gin, gsum, ptop, ct, part, rin, part2, rsum, st, zpart, h_s, b_s, r_s, u_s, cmx,
                  csem, psem, zsend, zrecv, osem, gsend, grecv, tsend, trecv, csend, crecv, r1sem, r2send, r2recv,
                  casend, carecv, sasend, sarecv, msem):
    cbuf = out.at[pl.ds(0, TRAIL), :]
    me = lax.axis_index('pr')
    q = lax.axis_index('pc')
    core = lax.rem(me, 2)
    chip = (me - core) // 2
    twin = me + 1 - 2 * core
    partner = {'pc': 1 - q}
    mine = pl.ds(pl.multiple_of(q * NB, NB), NB)
    theirs = pl.ds(pl.multiple_of((1 - q) * NB, NB), NB)

    def remote(src, dst, s_sem, r_sem, dev):
        return pltpu.make_async_remote_copy(src_ref=src, dst_ref=dst, send_sem=s_sem, recv_sem=r_sem, device_id=dev, device_id_type=MESH)

    def lanes(c):
        return pl.ds(c * LANES, LANES)

    def load_trail(c):
        return pltpu.make_async_copy(trail_hbm.at[:, lanes(c)], cbuf.at[:, lanes(c)], csem.at[c])

    def load_panel(c):
        return pltpu.make_async_copy(panel_hbm.at[:, lanes(c)], pt.at[mine, lanes(c)], psem.at[c])

    def send_panel(c):
        return remote(pt.at[mine, lanes(c)], pt.at[mine, lanes(c)], zsend.at[c], zrecv.at[c], partner)

    def recv_panel(c):
        return remote(pt.at[theirs, lanes(c)], pt.at[theirs, lanes(c)], zsend.at[c], zrecv.at[c], partner)

    for c in range(NCH):
        load_panel(c).start()
    for c in range(NCH):
        load_trail(c).start()

    barrier = pltpu.get_barrier_semaphore()
    pl.semaphore_signal(barrier, inc=1, device_id=partner, device_id_type=MESH)
    for d in range(1, NPR):
        pl.semaphore_signal(barrier, inc=1, device_id={'pr': lax.rem(me + d, NPR)}, device_id_type=MESH)
    pl.semaphore_wait(barrier, NPR)
    for c in range(NCH):
        load_panel(c).wait()
        send_panel(c).start()

    def piece(buf, i):
        return buf.at[pl.ds(pl.multiple_of(i * OWN, 8), OWN), :]

    def gather_start(buf, ssem, rsem):
        for d in range(4):
            dev = twin if d == 0 else lax.rem(me + 2 * d, NPR)
            remote(piece(buf, me), piece(buf, me), ssem.at[d], rsem.at[me], {'pr': dev}).start()

    def gather_forward(buf, ssem, rsem):
        for d in range(1, 4):
            src = lax.rem(me + NPR - 2 * d, NPR)
            remote(piece(buf, src), piece(buf, src), ssem.at[3 + d], rsem.at[src], {'pr': twin}).wait_recv()
            remote(piece(buf, src), piece(buf, src), ssem.at[3 + d], rsem.at[src], {'pr': twin}).start()

    def gather_wait(buf, ssem, rsem):
        for d in range(4):
            src = lax.rem(twin + NPR - 2 * d, NPR)
            remote(piece(buf, src), piece(buf, src), ssem.at[d], rsem.at[src], {'pr': twin}).wait_recv()

    def gather_end(buf, ssem, rsem):
        for d in range(7):
            remote(piece(buf, me), piece(buf, me), ssem.at[d], rsem.at[me], {'pr': twin}).wait_send()

    def share_top(i):
        return remote(pt.at[:, pl.ds(0, NP)], ptop, tsend.at[i], trecv, {'pr': i})

    def scatter_top(i):
        return remote(cbuf.at[pl.ds(i * OWN, OWN), pl.ds(0, NP)], piece(ct, i), csend.at[i], crecv, {'pr': i})

    part[...] = jnp.zeros_like(part)
    gown[...] = jnp.zeros_like(gown)

    def make_pieces(c):
        hi, mid, low = split3(pt[:, lanes(c)].T)
        pp[:, :NP] = hi
        pp[:, NP:2 * NP] = mid
        pp[:, 2 * NP:] = low
        gown[:NP, :] += dot_parts(pt[:, lanes(c)], pp[...])

    def product(c, first, last):
        def rows_step(m, carry):
            rows = pl.ds(pl.multiple_of(m * MROWS, MROWS), MROWS)
            got = dot_parts(cbuf[rows, lanes(c)], pp[...])
            part[m] += got.reshape(2, OWN, NP)
            return carry

        lax.fori_loop(first, last, rows_step, 0)

    cmax = jnp.zeros((8, LANES), jnp.float32)
    for c in range(NCH):
        load_trail(c).wait()
        if c == 0:
            @pl.when(me == 0)
            def _():
                ct[:OWN, :] = cbuf[:OWN, :NP]
                for i in range(1, NPR):
                    scatter_top(i).start()

        def largest(m, acc):
            x = cbuf[pl.ds(pl.multiple_of(m * OWN, OWN), OWN), lanes(c)]
            return jnp.maximum(acc, jnp.max(jnp.abs(x).reshape(OWN // 8, 8, LANES), axis=0))

        cmax = lax.fori_loop(0, NPR, largest, cmax)
        if c == 1:
            @pl.when(me != 0)
            def _():
                remote(piece(ct, me), piece(ct, me), csend.at[0], crecv, {'pr': 0}).wait_recv()

            gather_start(ct, casend, carecv)
        if c == 3:
            gather_forward(ct, casend, carecv)
        recv_panel(c).wait_recv()
        if c == 0:
            @pl.when(me == 0)
            def _():
                ptop[...] = pt[:, :NP]
                for i in range(1, NPR):
                    share_top(i).start()
        make_pieces(c)
        if c < NCH - 1:
            product(c, 0, 4)

    big = jnp.max(jnp.max(cmax, axis=1, keepdims=True), axis=0, keepdims=True)
    gown[NP:, :] = jnp.broadcast_to(big, (8, NP))

    gcopy = remote(gown, gin, gsend.at[0], grecv.at[4], {'pr': twin})
    gcopy.start()
    product(NCH - 1, 0, 2)
    gcopy.wait()
    gsum[chip, :NP, :] = gown[:NP, :] + gin[:NP, :]
    gsum[chip, NP:, :] = jnp.maximum(gown[NP:, :], gin[NP:, :])

    def send_gram(d):
        return remote(gsum.at[chip], gsum.at[chip], gsend.at[d], grecv.at[chip], {'pr': lax.rem(me + 2 * d, NPR)})

    for d in range(1, 4):
        send_gram(d).start()
    pt_copy = pltpu.make_async_copy(pt, pt_out, osem)
    pt_copy.start()
    product(NCH - 1, 2, 4)

    scopy = remote(part.at[:, 1 - core], rin, r1sem.at[0], r1sem.at[1], {'pr': twin})
    scopy.start()

    @pl.when(me != 0)
    def _():
        remote(ptop, ptop, tsend.at[0], trecv, {'pr': 0}).wait_recv()

    for d in range(1, 4):
        src = lax.rem(chip + 4 - d, 4)
        remote(gsum.at[src], gsum.at[src], gsend.at[d], grecv.at[src], {'pr': twin}).wait_recv()
    gram = ((gsum[0, :NP, :] + gsum[1, :NP, :]) + gsum[2, :NP, :]) + gsum[3, :NP, :]
    cmx[0] = jnp.maximum(jnp.maximum(gsum[0, NP:, :], gsum[1, NP:, :]), jnp.maximum(gsum[2, NP:, :], gsum[3, NP:, :]))
    mcopy = remote(cmx.at[0], cmx.at[1], msem.at[0], msem.at[1], partner)
    mcopy.start()

    eyeb = eye_of(NP)
    eye = jnp.where(eyeb, 1.0, 0.0)
    row_id = lax.broadcasted_iota(jnp.int32, (NP, NP), 0)
    col_id = lax.broadcasted_iota(jnp.int32, (NP, NP), 1)

    def newton_rsqrt(x):
        y = lax.rsqrt(x)
        return y * (1.5 - 0.5 * x * y * y)

    gdiag = jnp.where(eyeb, gram, 0.0)
    g_row = jnp.sum(gdiag, axis=0, keepdims=True)
    g_col = jnp.sum(gdiag, axis=1, keepdims=True)
    n_row, n_col = newton_rsqrt(g_row), newton_rsqrt(g_col)
    h_s[...] = (gram * n_row) * n_col
    b_s[...] = ptop[...].T * n_row
    factor_steps(h_s, b_s, r_s, u_s, 0, 0, 16)

    scopy.wait()
    for s in range(4):
        part2[s] = part[s, core] + rin[s]

    def scatter_part(d):
        to = lax.rem(chip + d, 4)
        return remote(part2.at[to], rsum.at[chip], r2send.at[d], r2recv.at[chip], {'pr': 2 * to + core})

    for d in range(1, 4):
        scatter_part(d).start()
    factor_steps(h_s, b_s, r_s, u_s, 0, 16, 64)
    rsum[chip] = part2[chip]
    for d in range(1, 4):
        src = lax.rem(chip + 4 - d, 4)
        remote(part2.at[src], rsum.at[src], r2send.at[d], r2recv.at[src], {'pr': twin}).wait_recv()
    st[pl.ds(pl.multiple_of(me * OWN, 8), OWN), :] = ((rsum[0] + rsum[1]) + rsum[2]) + rsum[3]
    gather_start(st, sasend, sarecv)
    factor_steps(h_s, b_s, r_s, u_s, NB, 64, 120)
    gather_forward(st, sasend, sarecv)
    gather_wait(ct, casend, carecv)
    factor_steps(h_s, b_s, r_s, u_s, NB, 120, 128)

    rmat, umat = r_s[...], u_s[...]
    lstrict = jnp.where(row_id > col_id, b_s[...], 0.0)
    lmat = eye + lstrict

    def upper_inv(mat):
        diag = jnp.where(eyeb, mat, 0.0)
        d_row = 1.0 / jnp.sum(diag, axis=0, keepdims=True)
        d_col = 1.0 / jnp.sum(diag, axis=1, keepdims=True)
        return unit_tri_inv(jnp.where(col_id > row_id, -(mat * d_col), 0.0), eye) * d_row

    rinv = upper_inv(rmat)
    uinv = upper_inv(umat)
    linv = unit_tri_inv(-lstrict, eye)
    out[AUX0:, WT0:WT0 + NP] = (uinv * n_col).T
    linv_t = linv.T
    m2_t = (fdot(linv, rinv.T) * n_row).T
    out[AUX0:AUX0 + 8, TAU0:TAU0 + NP] = jnp.broadcast_to(jnp.sum(jnp.where(eyeb, -umat / rmat, 0.0), axis=0, keepdims=True), (8, NP))
    out[AUX0:, TOP0:TOP0 + NP] = lmat.T
    out[AUX0:, TOP1:TOP1 + NP] = jnp.where(row_id > col_id, lmat, rmat * (g_row * n_row)).T

    mcopy.wait()
    c_top = jnp.max(jnp.maximum(cmx[0], cmx[1]), axis=1, keepdims=True)[:1]
    g_max = jnp.max(g_row, axis=1, keepdims=True)
    g_min = jnp.min(g_row, axis=1, keepdims=True)

    def total_of(x):
        return jnp.sum(jnp.sum(x, axis=1, keepdims=True), axis=0, keepdims=True)

    resid = total_of(jnp.abs(fdot(rinv, rmat) - eye) + jnp.abs(fdot(uinv, umat) - eye) + jnp.abs(fdot(linv, lmat) - eye))
    cond = total_of(rinv * rinv + uinv * uinv + linv * linv)
    good = (g_max < 1e12) & (g_min > 1e-12) & (resid < 1e-3) & (cond < 2048.0)
    good = good & (c_top < 1e26) & ((c_top > 1e-20) | (c_top == 0.0))
    out[AUX0:AUX0 + 8, BAD0:BAD0 + NP] = jnp.broadcast_to(jnp.where(good, 0.0, 1.0), (8, NP))

    gather_wait(st, sasend, sarecv)

    for b in range(4):
        rows = slice(b * MROWS, (b + 1) * MROWS)
        zpart[rows, :] = fdot(ct[rows, :], linv_t) - fdot(st[rows, :], m2_t)
    for b in range(16):
        n = min(NP, TRAIL - b * NP)
        out[AUX0:AUX0 + n, b * NP:(b + 1) * NP] = zpart[b * NP:b * NP + n, :]

    for c in range(NCH):
        send_panel(c).wait_send()
    pt_copy.wait()
    gather_end(ct, casend, carecv)
    gather_end(st, sasend, sarecv)
    for d in range(1, 4):
        send_gram(d).wait_send()
        scatter_part(d).wait_send()

    @pl.when(me == 0)
    def _():
        for i in range(1, NPR):
            share_top(i).wait_send()
            scatter_top(i).wait_send()


def reduce_call(panel_t, trail_t):
    f32 = jnp.float32
    dma = pltpu.SemaphoreType.DMA
    vmem = pl.BlockSpec(memory_space=pltpu.VMEM)
    hbm = pl.BlockSpec(memory_space=pl.ANY)
    return pl.pallas_call(
        reduce_kernel,
        out_shape=(pltpu.VMEM((ALL, ROWS), f32), pltpu.HBM((NP, ROWS), f32)),
        in_specs=[hbm, hbm],
        out_specs=(vmem, hbm),
        scratch_shapes=[
            pltpu.VMEM((NP, ROWS), f32), pltpu.VMEM((LANES, 3 * NP), jnp.bfloat16),
            pltpu.VMEM((MSG, NP), f32), pltpu.VMEM((MSG, NP), f32), pltpu.VMEM((4, MSG, NP), f32), pltpu.VMEM((NP, NP), f32),
            pltpu.VMEM((TRAIL, NP), f32), pltpu.VMEM((4, 2, OWN, NP), f32), pltpu.VMEM((4, OWN, NP), f32), pltpu.VMEM((4, OWN, NP), f32),
            pltpu.VMEM((4, OWN, NP), f32), pltpu.VMEM((TRAIL, NP), f32), pltpu.VMEM((TRAIL, NP), f32),
            pltpu.VMEM((NP, NP), f32), pltpu.VMEM((NP, NP), f32), pltpu.VMEM((NP, NP), f32), pltpu.VMEM((NP, NP), f32), pltpu.VMEM((2, 8, NP), f32),
            dma((NCH,)), dma((NCH,)), dma((NCH,)), dma((NCH,)), dma(()), dma((4,)), dma((5,)), dma((NPR,)), dma(()), dma((NPR,)), dma(()),
            dma((2,)), dma((4,)), dma((4,)), dma((7,)), dma((NPR,)), dma((7,)), dma((NPR,)), dma((2,))],
        compiler_params=pltpu.CompilerParams(collective_id=0, has_side_effects=True, vmem_limit_bytes=18 << 20),
        name='reduce',
    )(pltpu.with_memory_space_constraint(panel_t, pltpu.HBM), pltpu.with_memory_space_constraint(trail_t, pltpu.HBM))


UL = 512
NUL = ROWS // UL


def update_kernel(c_ref, pt_hbm, o_hbm, pan_hbm, tau_out, bad_out, pt, zcat, va, vb, sa, sb, pan, osem, psem, isem):
    q = lax.axis_index('pc')
    head = pltpu.make_async_copy(pt_hbm.at[:, :UL], pt.at[:, :UL], isem.at[0])
    tail = pltpu.make_async_copy(pt_hbm.at[:, UL:], pt.at[:, UL:], isem.at[1])
    head.start()
    tail.start()
    for b in range(16):
        rows = min(NP, TRAIL - b * NP)
        zh, zm, zl = split3(c_ref[AUX0:AUX0 + rows, b * NP:(b + 1) * NP])
        for n, piece in enumerate((zh, zh, zm, zm, zl, zh)):
            zcat[b * NP:b * NP + rows, n * NP:(n + 1) * NP] = piece
    tau_out[...] = c_ref[AUX0:AUX0 + 1, TAU0:TAU0 + NP]
    bad_out[...] = c_ref[AUX0:AUX0 + 1, BAD0:BAD0 + NP]

    def tile(i):
        return pl.ds(pl.multiple_of(i * UL, UL), UL)

    def make_v(i, vcat, first=False):
        v = fdot(c_ref[AUX0:, WT0:WT0 + NP], pt[:, tile(i)])
        stored = v
        if first:
            inside = (lax.broadcasted_iota(jnp.int32, (NP, UL), 1) < NP) & (lax.axis_index('pr') == 0)
            pad = jnp.zeros((NP, UL - NP), jnp.float32)
            stored = jnp.where(inside, jnp.concatenate([c_ref[AUX0:, TOP1:TOP1 + NP], pad], axis=1), v)
            v = jnp.where(inside, jnp.concatenate([c_ref[AUX0:, TOP0:TOP0 + NP], pad], axis=1), v)
        pan[:, tile(i)] = jnp.where(q == 0, stored[:NB], stored[NB:])
        vh, vm, vl = split3(v)
        for n, piece in enumerate((vh, vm, vh, vm, vh, vl)):
            vcat[n * NP:(n + 1) * NP, :] = piece

    def make_out(i, vcat, stage):
        for m in range(TRAIL // MROWS):
            rows = slice(m * MROWS, (m + 1) * MROWS)
            stage[rows, :] = c_ref[rows, tile(i)] - bdot(zcat[rows, :], vcat[...])

    def put(i, stage, k):
        return pltpu.make_async_copy(stage, o_hbm.at[:, tile(i)], osem.at[k])

    head.wait()
    make_v(0, va, True)
    tail.wait()

    def pair(p, carry):
        i = 2 * p

        @pl.when(p > 0)
        def _():
            put(i, sa, 0).wait()

        make_v(i + 1, vb)
        make_out(i, va, sa)
        put(i, sa, 0).start()

        @pl.when(p > 0)
        def _():
            put(i, sb, 1).wait()

        make_v(jnp.minimum(i + 2, NUL - 1), va)
        make_out(i + 1, vb, sb)
        put(i + 1, sb, 1).start()
        return carry

    lax.fori_loop(0, NUL // 2, pair, 0)
    pan_copy = pltpu.make_async_copy(pan, pan_hbm, psem)
    pan_copy.start()
    put(0, sa, 0).wait()
    put(0, sb, 1).wait()
    pan_copy.wait()


def update_call(work, pt):
    f32 = jnp.float32
    vmem = pl.BlockSpec(memory_space=pltpu.VMEM)
    hbm = pl.BlockSpec(memory_space=pl.ANY)
    return pl.pallas_call(
        update_kernel,
        out_shape=(jax.ShapeDtypeStruct((TRAIL, ROWS), f32), jax.ShapeDtypeStruct((NB, ROWS), f32), jax.ShapeDtypeStruct((1, NP), f32), jax.ShapeDtypeStruct((1, NP), f32)),
        in_specs=[vmem, hbm],
        out_specs=(hbm, hbm, vmem, vmem),
        scratch_shapes=[
            pltpu.VMEM((NP, ROWS), f32), pltpu.VMEM((TRAIL, 6 * NP), jnp.bfloat16), pltpu.VMEM((6 * NP, UL), jnp.bfloat16), pltpu.VMEM((6 * NP, UL), jnp.bfloat16),
            pltpu.VMEM((TRAIL, UL), f32), pltpu.VMEM((TRAIL, UL), f32), pltpu.VMEM((NB, ROWS), f32),
            pltpu.SemaphoreType.DMA((2,)), pltpu.SemaphoreType.DMA(()), pltpu.SemaphoreType.DMA((2,))],
        compiler_params=pltpu.CompilerParams(vmem_limit_bytes=20 << 20),
        name='update',
    )(work, pltpu.with_memory_space_constraint(pt, pltpu.HBM))


def sum_rows(x):
    for bit in (1, 2, 4):
        x = x + lax.ppermute(x, 'pr', [(i, i ^ bit) for i in range(NPR)])
    return x


def from_owner(x, owner):
    x = jnp.where(lax.axis_index('pc') == owner, x, 0.0)
    return x + lax.ppermute(x, 'pc', [(0, 1), (1, 0)])


def factor_panel(panel_blk, row_ids, first_row):
    col_ids = jnp.arange(NB)

    def column_step(j, carry):
        fac_panel, tau_vec = carry
        diag_row = first_row + j
        column = lax.dynamic_slice_in_dim(fac_panel, j, 1, axis=1)[:, 0]
        below_diag = row_ids > diag_row
        at_diag = row_ids == diag_row
        stats = sum_rows(jnp.stack([jnp.sum(jnp.where(row_ids >= diag_row, column * column, 0.0)), jnp.sum(jnp.where(at_diag, column, 0.0))]))
        diag_val = stats[1]
        col_norm = jnp.sqrt(stats[0])
        beta_val = jnp.where(diag_val >= 0.0, -col_norm, col_norm)
        tau_j = (beta_val - diag_val) / beta_val
        house_vec = jnp.where(below_diag, column / (diag_val - beta_val), jnp.where(at_diag, 1.0, 0.0))
        proj_row = sum_rows(jnp.sum(house_vec[:, None] * fac_panel, axis=0))
        proj_row = jnp.where(col_ids > j, tau_j * proj_row, 0.0)
        fac_panel = fac_panel - house_vec[:, None] * proj_row[None, :]
        new_col = jnp.where(below_diag, house_vec, jnp.where(at_diag, beta_val, column))
        fac_panel = jnp.where(col_ids[None, :] == j, new_col[:, None], fac_panel)
        return fac_panel, jnp.where(col_ids == j, tau_j, tau_vec)

    return lax.fori_loop(0, NB, column_step, (panel_blk, jnp.zeros((NB,), jnp.float32)))


def build_t(gram_mat, tau_vec):
    col_ids = jnp.arange(NB)

    def t_step(j, t_mat):
        g_col = jnp.where(col_ids < j, lax.dynamic_slice_in_dim(gram_mat, j, 1, axis=1)[:, 0], 0.0)
        tau_j = jnp.sum(jnp.where(col_ids == j, tau_vec, 0.0))
        new_col = jnp.where(col_ids == j, tau_j, -tau_j * jnp.sum(t_mat * g_col[None, :], axis=1))
        return jnp.where(col_ids[None, :] == j, new_col[:, None], t_mat)

    return lax.fori_loop(0, NB, t_step, jnp.zeros((NB, NB), jnp.float32))


def by_columns(panel, trail, shift):
    col_idx = lax.axis_index('pc')
    row_ids = lax.axis_index('pr') * ROWS + jnp.arange(ROWS) + shift
    taus = []
    for k in range(2):
        fac_panel, tau_vec = factor_panel(panel, row_ids, k * NB)
        diag = k * NB + jnp.arange(NB)
        v_mat = jnp.where(row_ids[:, None] > diag[None, :], fac_panel, jnp.where(row_ids[:, None] == diag[None, :], 1.0, 0.0))
        v_mat = from_owner(v_mat, k)
        tau_vec = from_owner(tau_vec, k)
        t_mat = build_t(sum_rows(mat_prod('rb,rc->bc', v_mat, v_mat)), tau_vec)

        def updated(cols):
            inner = mat_prod('bd,bc->dc', t_mat, sum_rows(mat_prod('rb,rc->bc', v_mat, cols)))
            return cols - mat_prod('rd,dc->rc', v_mat, inner)

        trail = updated(trail)
        later = updated(panel) if k == 0 else panel
        panel = jnp.where(col_idx == k, fac_panel, later)
        taus.append(tau_vec)
    return trail.T, panel.T, jnp.concatenate(taus)[None, :]


def solution(mesh):
    def local_run(panels_loc, trail_loc):
        panel_t = panels_loc.reshape(ROWS, NB).T
        trail_t = trail_loc.T
        trail_new, pan, tau, bad = update_call(*reduce_call(panel_t, trail_t))

        def again(state):
            shift = (state[0][0, 0] < 0.0).astype(jnp.int32)
            return (jnp.zeros_like(state[0]),) + by_columns(panel_t.T, trail_t.T, shift)

        _, trail_new, pan, tau = lax.while_loop(lambda s: s[0][0, 0] > 0.0, again, (bad, trail_new, pan, tau))
        return pan.T.reshape(ROWS, 1, NB), trail_new.T, tau.reshape(NP)

    return jax.shard_map(local_run, mesh=mesh, in_specs=(P('pr', 'pc', None), P('pr', 'pc')), out_specs=(P('pr', 'pc', None), P('pr', 'pc'), P()), check_vma=False)
```

```python
import jax
import jax.numpy as jnp
from jax import lax
from jax.experimental import pallas as pl
from jax.experimental.pallas import tpu as pltpu
from jax.sharding import PartitionSpec as P

FULL_PRECISION = lax.Precision.HIGHEST
MESH = pl.DeviceIdType.MESH
ROWS, NB, NP, TRAIL = 4096, 64, 128, 1984
NPR = 8
CHUNKS = ((0, 1024), (1024, 1024), (2048, 1024), (3072, 512), (3584, 512))
LANES = 1024
NCH = len(CHUNKS)
AUX0, ALL = TRAIL, TRAIL + NP
WT0, TOP0, TOP1, TAU0, BAD0 = (16 * NP, 17 * NP, 18 * NP, 19 * NP, 20 * NP)
OWN = TRAIL // NPR
MROWS = 496
MSG = NP + 8


def mat_prod(form, left, right):
    return jnp.einsum(form, left, right, precision=FULL_PRECISION, preferred_element_type=jnp.float32)


def fdot(a, b):
    return jnp.dot(a, b, precision=FULL_PRECISION, preferred_element_type=jnp.float32)


def bdot(a, b):
    return jnp.dot(a, b, preferred_element_type=jnp.float32)


def split3(x):
    hi = x.astype(jnp.bfloat16)
    rest = x - hi.astype(jnp.float32)
    mid = rest.astype(jnp.bfloat16)
    low = (rest - mid.astype(jnp.float32)).astype(jnp.bfloat16)
    return hi, mid, low


def dot_parts(x, pieces):
    hi, mid, low = split3(x)
    d1 = bdot(hi, pieces)
    d2 = bdot(mid, pieces[:, :2 * NP])
    d3 = bdot(low, pieces[:, :NP])
    return d1[:, :NP] + ((d1[:, NP:2 * NP] + d2[:, :NP]) + ((d1[:, 2 * NP:] + d3) + d2[:, NP:]))


def unit_tri_inv(strict, eye):
    n = strict.shape[0]
    inv = eye + strict
    power = fdot(strict, strict)
    for _ in range(5):
        both = dot_parts(jnp.concatenate([inv, power], axis=0), jnp.concatenate(split3(power), axis=1))
        inv = inv + both[:n]
        power = both[n:]
    return inv + fdot(inv, power)


def eye_of(n):
    return lax.broadcasted_iota(jnp.int32, (n, n), 0) == lax.broadcasted_iota(jnp.int32, (n, n), 1)


def column_of(ref, row0, j):
    return jnp.take_along_axis(ref[row0:, :], jnp.full((NP - row0, NP), j, jnp.int32), axis=1)


def factor_steps(h_s, b_s, r_s, u_s, hc_s, bc_s, bn_s, row0, start, stop):
    lane1 = lax.broadcasted_iota(jnp.int32, (1, NP), 1)
    lane = lax.broadcasted_iota(jnp.int32, (NP - row0, NP), 1)

    def step(j, carry):
        after = jnp.minimum(j + 1, NP - 1)
        hnext = column_of(h_s, row0, after)
        bnext = column_of(b_s, row0, after)
        bn_s[row0:, :] = bnext
        hcol, bcol = hc_s[row0:, :], bc_s[row0:, :]
        hjj, alpha = hc_s[pl.ds(j, 1), :], bc_s[pl.ds(j, 1), :]
        hjn, bjn = hc_s[pl.ds(after, 1), :], bn_s[pl.ds(j, 1), :]
        hrow, brow = h_s[pl.ds(j, 1), :], b_s[pl.ds(j, 1), :]
        root = lax.rsqrt(hjj)
        root = root * (1.5 - 0.5 * hjj * root * root)
        beta = jnp.where(alpha >= 0.0, -hjj * root, hjj * root)
        invb = jnp.where(alpha >= 0.0, -root, root)
        invd = 1.0 / (alpha - beta)
        keep = lane1 >= j
        rrow = jnp.where(keep, hrow * invb, 0.0)
        urow = jnp.where(keep, brow - rrow, 0.0)
        r_s[pl.ds(j, 1), :] = rrow
        u_s[pl.ds(j, 1), :] = urow
        vcol = bcol * invd
        hc_s[row0:, :] = hnext - hcol * (hjn * invb * invb)
        bc_s[row0:, :] = bnext - vcol * (bjn - hjn * invb)
        h_s[row0:, :] = h_s[row0:, :] - hcol * (rrow * invb)
        b_s[row0:, :] = jnp.where(lane == j, vcol, b_s[row0:, :] - vcol * urow)
        return carry

    def four(g, carry):
        for i in range(4):
            step(start + 4 * g + i, carry)
        return carry

    lax.fori_loop(0, (stop - start) // 4, four, 0)


def reduce_kernel(panel_hbm, trail_hbm, out, pt_out,
                  pt, pp, gown, gin, gsum, ptop, ct, part, rin, part2, rsum, st, zpart, h_s, b_s, r_s, u_s, hc_s, bc_s, bn_s, cmx,
                  csem, psem, zsend, zrecv, osem, gsend, grecv, tsend, trecv, csend, crecv, r1sem, r2send, r2recv,
                  casend, carecv, sasend, sarecv, msem):
    cbuf = out.at[pl.ds(0, TRAIL), :]
    me = lax.axis_index('pr')
    q = lax.axis_index('pc')
    core = lax.rem(me, 2)
    chip = (me - core) // 2
    twin = me + 1 - 2 * core
    partner = {'pc': 1 - q}
    mine = pl.ds(pl.multiple_of(q * NB, NB), NB)
    theirs = pl.ds(pl.multiple_of((1 - q) * NB, NB), NB)

    def remote(src, dst, s_sem, r_sem, dev):
        return pltpu.make_async_remote_copy(src_ref=src, dst_ref=dst, send_sem=s_sem, recv_sem=r_sem, device_id=dev, device_id_type=MESH)

    def lanes(c):
        return pl.ds(*CHUNKS[c])

    def load_trail(c):
        return pltpu.make_async_copy(trail_hbm.at[:, lanes(c)], cbuf.at[:, lanes(c)], csem.at[c])

    def load_panel(c):
        return pltpu.make_async_copy(panel_hbm.at[:, lanes(c)], pt.at[mine, lanes(c)], psem.at[c])

    def send_panel(c):
        return remote(pt.at[mine, lanes(c)], pt.at[mine, lanes(c)], zsend.at[c], zrecv.at[c], partner)

    def recv_panel(c):
        return remote(pt.at[theirs, lanes(c)], pt.at[theirs, lanes(c)], zsend.at[c], zrecv.at[c], partner)

    for c in range(NCH):
        load_panel(c).start()
    for c in range(NCH):
        load_trail(c).start()

    barrier = pltpu.get_barrier_semaphore()
    pl.semaphore_signal(barrier, inc=1, device_id=partner, device_id_type=MESH)
    for d in range(1, NPR):
        pl.semaphore_signal(barrier, inc=1, device_id={'pr': lax.rem(me + d, NPR)}, device_id_type=MESH)
    pl.semaphore_wait(barrier, NPR)
    for c in range(NCH):
        load_panel(c).wait()
        send_panel(c).start()

    def piece(buf, i):
        return buf.at[pl.ds(pl.multiple_of(i * OWN, 8), OWN), :]

    def gather_start(buf, ssem, rsem):
        for d in range(4):
            dev = twin if d == 0 else lax.rem(me + 2 * d, NPR)
            remote(piece(buf, me), piece(buf, me), ssem.at[d], rsem.at[me], {'pr': dev}).start()

    def gather_forward(buf, ssem, rsem):
        for d in range(1, 4):
            src = lax.rem(me + NPR - 2 * d, NPR)
            remote(piece(buf, src), piece(buf, src), ssem.at[3 + d], rsem.at[src], {'pr': twin}).wait_recv()
            remote(piece(buf, src), piece(buf, src), ssem.at[3 + d], rsem.at[src], {'pr': twin}).start()

    def gather_wait(buf, ssem, rsem):
        for d in range(4):
            src = lax.rem(twin + NPR - 2 * d, NPR)
            remote(piece(buf, src), piece(buf, src), ssem.at[d], rsem.at[src], {'pr': twin}).wait_recv()

    def gather_end(buf, ssem, rsem):
        for d in range(7):
            remote(piece(buf, me), piece(buf, me), ssem.at[d], rsem.at[me], {'pr': twin}).wait_send()

    def share_top(i):
        return remote(pt.at[:, pl.ds(0, NP)], ptop, tsend.at[i], trecv, {'pr': i})

    def scatter_top(i):
        return remote(cbuf.at[pl.ds(i * OWN, OWN), pl.ds(0, NP)], piece(ct, i), csend.at[i], crecv, {'pr': i})

    part[...] = jnp.zeros_like(part)
    gown[...] = jnp.zeros_like(gown)

    def make_pieces(c):
        n = CHUNKS[c][1]
        hi, mid, low = split3(pt[:, lanes(c)].T)
        pp[:n, :NP] = hi
        pp[:n, NP:2 * NP] = mid
        pp[:n, 2 * NP:] = low
        gown[:NP, :] += dot_parts(pt[:, lanes(c)], pp[:n, :])

    def product(c, first, last):
        def rows_step(m, carry):
            rows = pl.ds(pl.multiple_of(m * MROWS, MROWS), MROWS)
            got = dot_parts(cbuf[rows, lanes(c)], pp[:CHUNKS[c][1], :])
            part[m] += got.reshape(2, OWN, NP)
            return carry

        lax.fori_loop(first, last, rows_step, 0)

    cmax = jnp.zeros((8, 1), jnp.float32)
    for c in range(NCH):
        load_trail(c).wait()
        if c == 0:
            @pl.when(me == 0)
            def _():
                ct[:OWN, :] = cbuf[:OWN, :NP]
                for i in range(1, NPR):
                    scatter_top(i).start()

        def largest(m, acc):
            x = cbuf[pl.ds(pl.multiple_of(m * OWN, OWN), OWN), lanes(c)]
            return jnp.maximum(acc, jnp.max(jnp.abs(x).reshape(OWN // 8, 8, CHUNKS[c][1]), axis=0))

        most = lax.fori_loop(0, NPR, largest, jnp.zeros((8, CHUNKS[c][1]), jnp.float32))
        cmax = jnp.maximum(cmax, jnp.max(most, axis=1, keepdims=True))
        if c == 1:
            @pl.when(me != 0)
            def _():
                remote(piece(ct, me), piece(ct, me), csend.at[0], crecv, {'pr': 0}).wait_recv()

            gather_start(ct, casend, carecv)
        if c == 3:
            gather_forward(ct, casend, carecv)
        recv_panel(c).wait_recv()
        if c == 0:
            @pl.when(me == 0)
            def _():
                ptop[...] = pt[:, :NP]
                for i in range(1, NPR):
                    share_top(i).start()
        make_pieces(c)
        if c < NCH - 1:
            product(c, 0, 4)

    big = jnp.max(cmax, axis=0, keepdims=True)
    gown[NP:, :] = jnp.broadcast_to(big, (8, NP))

    gcopy = remote(gown, gin, gsend.at[0], grecv.at[4], {'pr': twin})
    gcopy.start()
    product(NCH - 1, 0, 2)
    gcopy.wait()
    gsum[chip, :NP, :] = gown[:NP, :] + gin[:NP, :]
    gsum[chip, NP:, :] = jnp.maximum(gown[NP:, :], gin[NP:, :])

    def send_gram(d):
        return remote(gsum.at[chip], gsum.at[chip], gsend.at[d], grecv.at[chip], {'pr': lax.rem(me + 2 * d, NPR)})

    for d in range(1, 4):
        send_gram(d).start()
    pt_copy = pltpu.make_async_copy(pt, pt_out, osem)
    pt_copy.start()
    product(NCH - 1, 2, 4)

    scopy = remote(part.at[:, 1 - core], rin, r1sem.at[0], r1sem.at[1], {'pr': twin})
    scopy.start()
    scopy.wait()
    for s in range(4):
        part2[s] = part[s, core] + rin[s]

    def scatter_part(d):
        to = lax.rem(chip + d, 4)
        return remote(part2.at[to], rsum.at[chip], r2send.at[d], r2recv.at[chip], {'pr': 2 * to + core})

    for d in range(1, 4):
        send_gram(d).wait_send()
    for d in range(1, 4):
        scatter_part(d).start()

    @pl.when(me != 0)
    def _():
        remote(ptop, ptop, tsend.at[0], trecv, {'pr': 0}).wait_recv()

    for d in range(1, 4):
        src = lax.rem(chip + 4 - d, 4)
        remote(gsum.at[src], gsum.at[src], gsend.at[d], grecv.at[src], {'pr': twin}).wait_recv()
    gram = ((gsum[0, :NP, :] + gsum[1, :NP, :]) + gsum[2, :NP, :]) + gsum[3, :NP, :]
    cmx[0] = jnp.maximum(jnp.maximum(gsum[0, NP:, :], gsum[1, NP:, :]), jnp.maximum(gsum[2, NP:, :], gsum[3, NP:, :]))
    mcopy = remote(cmx.at[0], cmx.at[1], msem.at[0], msem.at[1], partner)
    mcopy.start()

    eyeb = eye_of(NP)
    eye = jnp.where(eyeb, 1.0, 0.0)
    row_id = lax.broadcasted_iota(jnp.int32, (NP, NP), 0)
    col_id = lax.broadcasted_iota(jnp.int32, (NP, NP), 1)

    def newton_rsqrt(x):
        y = lax.rsqrt(x)
        return y * (1.5 - 0.5 * x * y * y)

    gdiag = jnp.where(eyeb, gram, 0.0)
    g_row = jnp.sum(gdiag, axis=0, keepdims=True)
    g_col = jnp.sum(gdiag, axis=1, keepdims=True)
    n_row, n_col = newton_rsqrt(g_row), newton_rsqrt(g_col)
    h_s[...] = (gram * n_row) * n_col
    b_s[...] = ptop[...].T * n_row
    hc_s[...] = column_of(h_s, 0, 0)
    bc_s[...] = column_of(b_s, 0, 0)
    factor_steps(h_s, b_s, r_s, u_s, hc_s, bc_s, bn_s, 0, 0, 64)
    rsum[chip] = part2[chip]
    for d in range(1, 4):
        src = lax.rem(chip + 4 - d, 4)
        remote(part2.at[src], rsum.at[src], r2send.at[d], r2recv.at[src], {'pr': twin}).wait_recv()
    st[pl.ds(pl.multiple_of(me * OWN, 8), OWN), :] = ((rsum[0] + rsum[1]) + rsum[2]) + rsum[3]
    gather_start(st, sasend, sarecv)
    factor_steps(h_s, b_s, r_s, u_s, hc_s, bc_s, bn_s, NB, 64, 128)
    gather_wait(ct, casend, carecv)

    rmat, umat = r_s[...], u_s[...]
    lstrict = jnp.where(row_id > col_id, b_s[...], 0.0)
    lmat = eye + lstrict

    def upper_inv(mat):
        diag = jnp.where(eyeb, mat, 0.0)
        d_row = 1.0 / jnp.sum(diag, axis=0, keepdims=True)
        d_col = 1.0 / jnp.sum(diag, axis=1, keepdims=True)
        return unit_tri_inv(jnp.where(col_id > row_id, -(mat * d_col), 0.0), eye) * d_row

    rinv = upper_inv(rmat)
    uinv = upper_inv(umat)
    linv = unit_tri_inv(-lstrict, eye)
    out[AUX0:, WT0:WT0 + NP] = (uinv * n_col).T
    linv_t = linv.T
    m2_t = (fdot(linv, rinv.T) * n_row).T
    out[AUX0:AUX0 + 8, TAU0:TAU0 + NP] = jnp.broadcast_to(jnp.sum(jnp.where(eyeb, -umat / rmat, 0.0), axis=0, keepdims=True), (8, NP))
    out[AUX0:, TOP0:TOP0 + NP] = lmat.T
    out[AUX0:, TOP1:TOP1 + NP] = jnp.where(row_id > col_id, lmat, rmat * (g_row * n_row)).T

    linv_pieces = jnp.concatenate(split3(linv_t), axis=1)
    m2_pieces = jnp.concatenate(split3(m2_t), axis=1)
    gather_forward(st, sasend, sarecv)
    for b in range(4):
        rows = slice(b * MROWS, (b + 1) * MROWS)
        zpart[rows, :] = dot_parts(ct[rows, :], linv_pieces)

    mcopy.wait()
    c_top = jnp.max(jnp.maximum(cmx[0], cmx[1]), axis=1, keepdims=True)[:1]
    g_max = jnp.max(g_row, axis=1, keepdims=True)
    g_min = jnp.min(g_row, axis=1, keepdims=True)

    def total_of(x):
        return jnp.sum(jnp.sum(x, axis=1, keepdims=True), axis=0, keepdims=True)

    resid = total_of(jnp.abs(fdot(rinv, rmat) - eye) + jnp.abs(fdot(uinv, umat) - eye) + jnp.abs(fdot(linv, lmat) - eye))
    cond = total_of(rinv * rinv + uinv * uinv + linv * linv)
    good = (g_max < 1e12) & (g_min > 1e-12) & (resid < 1e-3) & (cond < 2048.0)
    good = good & (c_top < 1e26) & ((c_top > 1e-20) | (c_top == 0.0))
    out[AUX0:AUX0 + 8, BAD0:BAD0 + NP] = jnp.broadcast_to(jnp.where(good, 0.0, 1.0), (8, NP))

    gather_wait(st, sasend, sarecv)

    for b in range(4):
        rows = slice(b * MROWS, (b + 1) * MROWS)
        zpart[rows, :] -= dot_parts(st[rows, :], m2_pieces)
    for b in range(16):
        n = min(NP, TRAIL - b * NP)
        out[AUX0:AUX0 + n, b * NP:(b + 1) * NP] = zpart[b * NP:b * NP + n, :]

    for c in range(NCH):
        send_panel(c).wait_send()
    pt_copy.wait()
    gather_end(ct, casend, carecv)
    gather_end(st, sasend, sarecv)
    for d in range(1, 4):
        scatter_part(d).wait_send()

    @pl.when(me == 0)
    def _():
        for i in range(1, NPR):
            share_top(i).wait_send()
            scatter_top(i).wait_send()


def reduce_call(panel_t, trail_t):
    f32 = jnp.float32
    dma = pltpu.SemaphoreType.DMA
    vmem = pl.BlockSpec(memory_space=pltpu.VMEM)
    hbm = pl.BlockSpec(memory_space=pl.ANY)
    return pl.pallas_call(
        reduce_kernel,
        out_shape=(pltpu.VMEM((ALL, ROWS), f32), pltpu.HBM((NP, ROWS), f32)),
        in_specs=[hbm, hbm],
        out_specs=(vmem, hbm),
        scratch_shapes=[
            pltpu.VMEM((NP, ROWS), f32), pltpu.VMEM((LANES, 3 * NP), jnp.bfloat16),
            pltpu.VMEM((MSG, NP), f32), pltpu.VMEM((MSG, NP), f32), pltpu.VMEM((4, MSG, NP), f32), pltpu.VMEM((NP, NP), f32),
            pltpu.VMEM((TRAIL, NP), f32), pltpu.VMEM((4, 2, OWN, NP), f32), pltpu.VMEM((4, OWN, NP), f32), pltpu.VMEM((4, OWN, NP), f32),
            pltpu.VMEM((4, OWN, NP), f32), pltpu.VMEM((TRAIL, NP), f32), pltpu.VMEM((TRAIL, NP), f32),
            pltpu.VMEM((NP, NP), f32), pltpu.VMEM((NP, NP), f32), pltpu.VMEM((NP, NP), f32), pltpu.VMEM((NP, NP), f32), pltpu.VMEM((NP, NP), f32), pltpu.VMEM((NP, NP), f32), pltpu.VMEM((NP, NP), f32), pltpu.VMEM((2, 8, NP), f32),
            dma((NCH,)), dma((NCH,)), dma((NCH,)), dma((NCH,)), dma(()), dma((4,)), dma((5,)), dma((NPR,)), dma(()), dma((NPR,)), dma(()),
            dma((2,)), dma((4,)), dma((4,)), dma((7,)), dma((NPR,)), dma((7,)), dma((NPR,)), dma((2,))],
        compiler_params=pltpu.CompilerParams(collective_id=0, has_side_effects=True, vmem_limit_bytes=18 << 20),
        name='reduce',
    )(pltpu.with_memory_space_constraint(panel_t, pltpu.HBM), pltpu.with_memory_space_constraint(trail_t, pltpu.HBM))


UL = 512
NUL = ROWS // UL


def update_kernel(c_ref, pt_hbm, o_hbm, pan_hbm, tau_out, bad_out, pt, zcat, va, vb, sa, sb, pan, osem, psem, isem):
    q = lax.axis_index('pc')
    head = pltpu.make_async_copy(pt_hbm.at[:, :UL], pt.at[:, :UL], isem.at[0])
    tail = pltpu.make_async_copy(pt_hbm.at[:, UL:], pt.at[:, UL:], isem.at[1])
    head.start()
    tail.start()
    for b in range(16):
        rows = min(NP, TRAIL - b * NP)
        zh, zm, zl = split3(c_ref[AUX0:AUX0 + rows, b * NP:(b + 1) * NP])
        for n, piece in enumerate((zh, zh, zm, zm, zl, zh)):
            zcat[b * NP:b * NP + rows, n * NP:(n + 1) * NP] = piece
    tau_out[...] = c_ref[AUX0:AUX0 + 1, TAU0:TAU0 + NP]
    bad_out[...] = c_ref[AUX0:AUX0 + 1, BAD0:BAD0 + NP]

    def tile(i):
        return pl.ds(pl.multiple_of(i * UL, UL), UL)

    def make_v(i, vcat, first=False):
        v = fdot(c_ref[AUX0:, WT0:WT0 + NP], pt[:, tile(i)])
        stored = v
        if first:
            inside = (lax.broadcasted_iota(jnp.int32, (NP, UL), 1) < NP) & (lax.axis_index('pr') == 0)
            pad = jnp.zeros((NP, UL - NP), jnp.float32)
            stored = jnp.where(inside, jnp.concatenate([c_ref[AUX0:, TOP1:TOP1 + NP], pad], axis=1), v)
            v = jnp.where(inside, jnp.concatenate([c_ref[AUX0:, TOP0:TOP0 + NP], pad], axis=1), v)
        pan[:, tile(i)] = jnp.where(q == 0, stored[:NB], stored[NB:])
        vh, vm, vl = split3(v)
        for n, piece in enumerate((vh, vm, vh, vm, vh, vl)):
            vcat[n * NP:(n + 1) * NP, :] = piece

    def make_out(i, vcat, stage):
        for m in range(TRAIL // MROWS):
            rows = slice(m * MROWS, (m + 1) * MROWS)
            stage[rows, :] = c_ref[rows, tile(i)] - bdot(zcat[rows, :], vcat[...])

    def put(i, stage, k):
        return pltpu.make_async_copy(stage, o_hbm.at[:, tile(i)], osem.at[k])

    head.wait()
    make_v(0, va, True)
    tail.wait()

    def pair(p, carry):
        i = 2 * p

        @pl.when(p > 0)
        def _():
            put(i, sa, 0).wait()

        make_v(i + 1, vb)
        make_out(i, va, sa)
        put(i, sa, 0).start()

        @pl.when(p > 0)
        def _():
            put(i, sb, 1).wait()

        make_v(jnp.minimum(i + 2, NUL - 1), va)
        make_out(i + 1, vb, sb)
        put(i + 1, sb, 1).start()
        return carry

    lax.fori_loop(0, NUL // 2, pair, 0)
    pan_copy = pltpu.make_async_copy(pan, pan_hbm, psem)
    pan_copy.start()
    put(0, sa, 0).wait()
    put(0, sb, 1).wait()
    pan_copy.wait()


def update_call(work, pt):
    f32 = jnp.float32
    vmem = pl.BlockSpec(memory_space=pltpu.VMEM)
    hbm = pl.BlockSpec(memory_space=pl.ANY)
    return pl.pallas_call(
        update_kernel,
        out_shape=(jax.ShapeDtypeStruct((TRAIL, ROWS), f32), jax.ShapeDtypeStruct((NB, ROWS), f32), jax.ShapeDtypeStruct((1, NP), f32), jax.ShapeDtypeStruct((1, NP), f32)),
        in_specs=[vmem, hbm],
        out_specs=(hbm, hbm, vmem, vmem),
        scratch_shapes=[
            pltpu.VMEM((NP, ROWS), f32), pltpu.VMEM((TRAIL, 6 * NP), jnp.bfloat16), pltpu.VMEM((6 * NP, UL), jnp.bfloat16), pltpu.VMEM((6 * NP, UL), jnp.bfloat16),
            pltpu.VMEM((TRAIL, UL), f32), pltpu.VMEM((TRAIL, UL), f32), pltpu.VMEM((NB, ROWS), f32),
            pltpu.SemaphoreType.DMA((2,)), pltpu.SemaphoreType.DMA(()), pltpu.SemaphoreType.DMA((2,))],
        compiler_params=pltpu.CompilerParams(vmem_limit_bytes=20 << 20),
        name='update',
    )(work, pltpu.with_memory_space_constraint(pt, pltpu.HBM))


def sum_rows(x):
    for bit in (1, 2, 4):
        x = x + lax.ppermute(x, 'pr', [(i, i ^ bit) for i in range(NPR)])
    return x


def from_owner(x, owner):
    x = jnp.where(lax.axis_index('pc') == owner, x, 0.0)
    return x + lax.ppermute(x, 'pc', [(0, 1), (1, 0)])


def factor_panel(panel_blk, row_ids, first_row):
    col_ids = jnp.arange(NB)

    def column_step(j, carry):
        fac_panel, tau_vec = carry
        diag_row = first_row + j
        column = lax.dynamic_slice_in_dim(fac_panel, j, 1, axis=1)[:, 0]
        below_diag = row_ids > diag_row
        at_diag = row_ids == diag_row
        stats = sum_rows(jnp.stack([jnp.sum(jnp.where(row_ids >= diag_row, column * column, 0.0)), jnp.sum(jnp.where(at_diag, column, 0.0))]))
        diag_val = stats[1]
        col_norm = jnp.sqrt(stats[0])
        beta_val = jnp.where(diag_val >= 0.0, -col_norm, col_norm)
        tau_j = (beta_val - diag_val) / beta_val
        house_vec = jnp.where(below_diag, column / (diag_val - beta_val), jnp.where(at_diag, 1.0, 0.0))
        proj_row = sum_rows(jnp.sum(house_vec[:, None] * fac_panel, axis=0))
        proj_row = jnp.where(col_ids > j, tau_j * proj_row, 0.0)
        fac_panel = fac_panel - house_vec[:, None] * proj_row[None, :]
        new_col = jnp.where(below_diag, house_vec, jnp.where(at_diag, beta_val, column))
        fac_panel = jnp.where(col_ids[None, :] == j, new_col[:, None], fac_panel)
        return fac_panel, jnp.where(col_ids == j, tau_j, tau_vec)

    return lax.fori_loop(0, NB, column_step, (panel_blk, jnp.zeros((NB,), jnp.float32)))


def build_t(gram_mat, tau_vec):
    col_ids = jnp.arange(NB)

    def t_step(j, t_mat):
        g_col = jnp.where(col_ids < j, lax.dynamic_slice_in_dim(gram_mat, j, 1, axis=1)[:, 0], 0.0)
        tau_j = jnp.sum(jnp.where(col_ids == j, tau_vec, 0.0))
        new_col = jnp.where(col_ids == j, tau_j, -tau_j * jnp.sum(t_mat * g_col[None, :], axis=1))
        return jnp.where(col_ids[None, :] == j, new_col[:, None], t_mat)

    return lax.fori_loop(0, NB, t_step, jnp.zeros((NB, NB), jnp.float32))


def by_columns(panel, trail, shift):
    col_idx = lax.axis_index('pc')
    row_ids = lax.axis_index('pr') * ROWS + jnp.arange(ROWS) + shift
    taus = []
    for k in range(2):
        fac_panel, tau_vec = factor_panel(panel, row_ids, k * NB)
        diag = k * NB + jnp.arange(NB)
        v_mat = jnp.where(row_ids[:, None] > diag[None, :], fac_panel, jnp.where(row_ids[:, None] == diag[None, :], 1.0, 0.0))
        v_mat = from_owner(v_mat, k)
        tau_vec = from_owner(tau_vec, k)
        t_mat = build_t(sum_rows(mat_prod('rb,rc->bc', v_mat, v_mat)), tau_vec)

        def updated(cols):
            inner = mat_prod('bd,bc->dc', t_mat, sum_rows(mat_prod('rb,rc->bc', v_mat, cols)))
            return cols - mat_prod('rd,dc->rc', v_mat, inner)

        trail = updated(trail)
        later = updated(panel) if k == 0 else panel
        panel = jnp.where(col_idx == k, fac_panel, later)
        taus.append(tau_vec)
    return trail.T, panel.T, jnp.concatenate(taus)[None, :]


def solution(mesh):
    def local_run(panels_loc, trail_loc):
        panel_t = panels_loc.reshape(ROWS, NB).T
        trail_t = trail_loc.T
        trail_new, pan, tau, bad = update_call(*reduce_call(panel_t, trail_t))

        def again(state):
            shift = (state[0][0, 0] < 0.0).astype(jnp.int32)
            return (jnp.zeros_like(state[0]),) + by_columns(panel_t.T, trail_t.T, shift)

        _, trail_new, pan, tau = lax.while_loop(lambda s: s[0][0, 0] > 0.0, again, (bad, trail_new, pan, tau))
        return pan.T.reshape(ROWS, 1, NB), trail_new.T, tau.reshape(NP)

    return jax.shard_map(local_run, mesh=mesh, in_specs=(P('pr', 'pc', None), P('pr', 'pc')), out_specs=(P('pr', 'pc', None), P('pr', 'pc'), P()), check_vma=False)
```
